32 devices in a mesh: grp: 4 (over x, core), dev: 8 (over z, y).
Axes of the slice: x: 2, y: 2, z: 4, core: 2. Of those that a mesh axis runs over, the one named last changes fastest.
Arguments:
- points: bfloat16 [65536, 1024], P(('grp', 'dev')), may hold values from -6 to 6
- blocks: int32 [65536, 1], P(('grp', 'dev')), may hold values from 0 to 63; in each aligned block of 2048 rows (0 to 2047, 2048 to 4095, ...) at most 64 rows name the same one
- finals: int32 [65536], P(('grp', 'dev')), may hold values from 0 to 255
- centroids: bfloat16 [16384, 1024], P('dev'), may hold values from -6 to 6
Outputs:
- distances: bfloat16 [65536, 256], P(('grp', 'dev'))
- refreshed_centroids: float32 [16384, 1024], P('dev', 'grp')
The draws below stay inside these ranges and needn't reach their ends.
Inputs may be any that keep to these rules, and one draw needn't show every extreme that they name: `blocks`: among the 2048 rows of one device no block is named by more than 64 rows, and some block by exactly 64. Block b is held by index b // 8 of dev. The point's centroid is row 256 * blocks + finals of centroids.
All inputs are finite; a program needn't handle non-finite values.
Results may differ from the reference program's by a relative error of at most 0.008.
Values may be sent and summed in bfloat16 or wider, within the bound.
A program may use at most 128 MiB of HBM per device.

```python
import math
import jax
import jax.numpy as jnp
import numpy as np
from jax import lax

D = 1024
BS = 256
POINTS_PER_SHARD = 2048
NB = 64
K = 16384
P_SIZE = 65536
MOST = 64
N_GRP = 4
N_DEV = 8


def place_ends(entries, own_key, smallest, top_value):
    dims = entries.shape
    index_at = [jax.random.randint(jax.random.fold_in(own_key, axis), (), 0, dims[axis]) for axis in range(len(dims))]
    entries = entries.at[tuple(index_at)].set(smallest)
    longest = dims.index(max(dims))
    index_at[longest] = (index_at[longest] + 1) % dims[longest]
    return entries.at[tuple(index_at)].set(top_value)


def shard_levels(stream_key, extent, cuts, smallest, top_value):
    def one(position, blocks):
        steps = jax.random.uniform(jax.random.fold_in(jax.random.fold_in(stream_key, 6), position), (blocks,), jnp.float32, smallest / len(cuts), top_value / len(cuts))
        return jnp.repeat(jnp.exp(steps), extent[position] // blocks).reshape((-1,) + (1,) * (len(extent) - position - 1))

    loudness = one(*cuts[0])
    for cut in cuts[1:]:
        loudness = loudness * one(*cut)
    return loudness


def assign_block(key, own, number, rows, count, top, most, skew):
    ranking = jax.random.permutation(key, count)
    heavy_load, usual = load_shares(count, rows * top, most, skew, True), load_shares(count, rows * top, most, skew, False)
    places = jnp.arange(count)

    def named(sizes, offset_by):
        used = int((sizes > 0).sum())
        fixed = max(1, used // 4)
        shifted = fixed + (places - fixed + offset_by * (used - fixed)) % max(1, count - fixed)
        return jnp.zeros((count,), jnp.int32).at[ranking[jnp.where(places < fixed, places, shifted)]].set(jnp.asarray(sizes, jnp.int32))

    sizes = jnp.where(number % 4 == 0, named(heavy_load, number // 4), named(usual, number - number // 4 - 1))
    mixed = jax.random.permutation(jax.random.fold_in(own, 3), count)
    giver, taker = mixed[0:count // 2 * 2:2], mixed[1:count // 2 * 2:2]
    margin = jnp.minimum(sizes[giver] - 1, most - sizes[taker]) // 2
    margin = jnp.where((giver == ranking[0]) | (taker == ranking[0]) | (sizes[taker] == 0), 0, jnp.maximum(margin, 0))
    shifted = jax.random.randint(jax.random.fold_in(own, 4), (count // 2,), 0, 1 << 20) % (margin + 1)
    sizes = sizes.at[giver].add(-shifted).at[taker].add(shifted)
    items = jnp.searchsorted(jnp.cumsum(sizes), jnp.arange(rows * top), side="right").astype(jnp.int32)
    grid = items.reshape(top, rows).T
    grid = grid[jax.random.permutation(jax.random.fold_in(own, 1), rows)]
    offset_by = jax.random.randint(jax.random.fold_in(own, 2), (rows, 1), 0, top)
    return jnp.take_along_axis(grid, (jnp.arange(top)[None, :] + offset_by) % top, axis=1)


def load_shares(amount, total, limit, slope, full):
    loads = [(1 << 20) // math.isqrt(rank ** slope) + 1 for rank in range(1, amount + 1)]
    largest = limit if full else min(limit, max(-(-total // amount), total * loads[0] // sum(loads)))
    least = 1 if total - largest >= amount - 1 else 0
    holding, surplus = [largest] + [least] * (amount - 1), total - largest - least * (amount - 1)
    while surplus > 0:
        free = [i for i in range(1, amount) if holding[i] < largest] or [i for i in range(1, amount) if holding[i] < limit]
        mass, left = sum([loads[i] for i in free]), surplus
        for i in free:
            extra = min(limit - holding[i], max(1, left * loads[i] // mass), surplus)
            holding[i] = holding[i] + extra
            surplus = surplus - extra
    return np.array(holding)


def normal_values(stream_key, dims, scale, bound, pieces=(), held_as=jnp.bfloat16):
    gain = shard_levels(stream_key, dims, pieces, -0.22, 0.18) if pieces else 1.0
    values = jax.random.normal(stream_key, dims, jnp.float32) * scale * gain
    return jnp.minimum(jnp.maximum(values, -bound), bound).astype(held_as)


def setup_inputs(seed: int = 0) -> dict:
    key_list = jax.random.split(jax.random.key(seed), 5)
    points = normal_values(key_list[0], (P_SIZE, D), 1.0, 6.0, ((0, 32),))
    blocks_keys = jax.random.split(jax.random.fold_in(key_list[1], 1), P_SIZE // POINTS_PER_SHARD)
    blocks_turns = jax.random.permutation(jax.random.fold_in(key_list[1], 3), P_SIZE // POINTS_PER_SHARD)
    blocks = jax.vmap(lambda own, number: assign_block(jax.random.fold_in(key_list[1], 2), own, number, POINTS_PER_SHARD, NB, 1, MOST, 2))(blocks_keys, blocks_turns).reshape((P_SIZE, 1))
    finals = place_ends(jax.random.randint(key_list[2], (P_SIZE,), 0, BS), jax.random.fold_in(key_list[2], 1), 0, BS - 1).astype(jnp.int32)
    centroids = normal_values(key_list[3], (K, D), 1.0, 6.0, ((0, 8),))
    return {"points": points, "blocks": blocks, "finals": finals, "centroids": centroids}


def reference(points, blocks, finals, centroids):
    npoints, width = points.shape
    nblocks = centroids.shape[0] // BS
    reach = N_GRP * N_DEV * MOST
    block_ids = blocks[:, 0].astype(jnp.int32)
    order = jnp.argsort(block_ids, stable=True).astype(jnp.int32)
    ordered = block_ids[order]
    labels = jnp.arange(nblocks, dtype=jnp.int32)
    starts = jnp.searchsorted(ordered, labels, side="left").astype(jnp.int32)
    stops = jnp.searchsorted(ordered, labels, side="right").astype(jnp.int32)
    padded = jnp.concatenate([order, jnp.zeros((reach,), jnp.int32)])
    columns = jnp.arange(BS, dtype=jnp.int32)
    positions = jnp.arange(reach, dtype=jnp.int32)

    def one_block(label):
        begin = starts[label]
        chosen = lax.dynamic_slice_in_dim(padded, begin, reach)
        live = positions < (stops[label] - begin)
        rows = points[chosen].astype(jnp.float32)
        centroid_table = lax.dynamic_slice_in_dim(centroids, (label * BS).astype(jnp.int32), BS, 0).astype(jnp.float32)
        cross_products = jnp.dot(rows, centroid_table.T, preferred_element_type=jnp.float32)
        dists = (jnp.sum(rows * rows, axis=1)[:, None] - 2.0 * cross_products + jnp.sum(centroid_table * centroid_table, axis=1)[None, :]) / width
        onehot_assign = jnp.where(live[:, None] & (finals[chosen][:, None] == columns[None, :]), 1.0, 0.0).astype(jnp.float32)
        sums = jnp.dot(onehot_assign.T, rows, preferred_element_type=jnp.float32)
        counts = jnp.sum(onehot_assign, axis=0)
        fresh = (sums + centroid_table) / (counts + 1.0)[:, None]
        where_to = jnp.where(live, chosen, npoints).astype(jnp.int32)
        return dists.astype(jnp.bfloat16), where_to, fresh

    dists, where_to, fresh = lax.map(one_block, labels)
    table = jnp.zeros((npoints + 1, BS), jnp.bfloat16).at[where_to.reshape(-1)].set(dists.reshape(-1, BS))
    return table[:npoints], fresh.reshape(nblocks * BS, width)
```

```python
import functools

import jax
import jax.numpy as jnp
from jax import lax
from jax.experimental import pallas as pl
from jax.experimental.pallas import tpu as pltpu
from jax.sharding import PartitionSpec as P

BS = 256
MSG = 128
MESH = pl.DeviceIdType.MESH
F32, BF16, I32 = jnp.float32, jnp.bfloat16, jnp.int32


def bits(n):
    return n.bit_length() - 1


def nt(a, b):
    return lax.dot_general(a, b, (((1,), (1,)), ((), ())), preferred_element_type=F32)


class Sizes:
    def __init__(self, n_grp, n_dev, npts, rows):
        self.g, self.dev = n_grp, n_dev
        self.nx = n_grp // 2
        ny = 1
        while 8 * ny * ny <= n_dev:
            ny *= 2
        self.ny, self.nz = ny, n_dev // ny
        self.team = n_grp * ny
        self.owned = rows // BS
        self.per = self.owned // n_grp
        self.n_blocks = self.owned * n_dev
        self.depth = 2 * npts // self.n_blocks
        self.steps = self.nz * self.per * self.depth // MSG
        self.zs = self.nz // self.steps
        self.nblk = self.zs * self.per
        self.line = self.nz == 4
        self.fins = 2 if self.line else self.nz - 1


def kernel(
    cf,
    block_row, final_row, points_hbm, cent_hbm,
    distances, fresh_out,
    points, tab, slot_row, slot_col, out, recv, tgt_out, tgt_in,
    part, own_sum, agg_in, fin_in, cnt, cagg_in, cfin_in,
    dist, ret, xs, xin,
    s_pts, r_pts, s_tgt, r_tgt, s_tab, r_tab, s_sum, r_agg, r_fin, s_cnt, r_cagg, r_cfin,
    s_ret, r_ret, s_x, r_x, in_sem,
):
    G, nx, ny, nz, TM = cf.g, cf.nx, cf.ny, cf.nz, cf.team
    per, depth, steps, zs, nblk = cf.per, cf.depth, cf.steps, cf.zs, cf.nblk
    g, d = lax.axis_index("grp"), lax.axis_index("dev")
    x, c = g // 2, g % 2
    z, y = d // ny, d % ny
    npts, width = points.shape
    share = width // G
    quarter = per * BS
    R = TM * MSG

    def to(gg, zz, yy):
        return {"grp": gg, "dev": zz * ny + yy}

    def split(o):
        return o // (2 * nx), o // 2 % nx, o % 2

    def mate(o):
        dy, dx, dc = split(o)
        return to((x + dx) % nx * 2 + (c + dc) % 2, z, (y + dy) % ny)

    def copy(src, dst, ss, rs, dev):
        return pltpu.make_async_remote_copy(
            src_ref=src, dst_ref=dst, send_sem=ss, recv_sem=rs, device_id=dev, device_id_type=MESH
        )

    half = z // (nz // 2)
    if cf.line:
        z_mate, z_inner, z_edge = half * 2 + 1 - z % 2, 2 - half, 3 * (1 - half)
        inner = (z + half) % 2 == 1
        edge = (z + half) % 2 == 0
        order = [z_edge, z_inner, z_mate, z]

    def zq(q):
        return order[q] if cf.line else (z + q + 1) % nz

    load_tab = pltpu.make_async_copy(
        cent_hbm.at[pl.ds(pl.multiple_of(g * quarter, quarter), quarter)], tab.at[z], in_sem.at[0]
    )
    load_points = pltpu.make_async_copy(points_hbm, points, in_sem.at[1])
    load_tab.start()
    load_points.start()

    barrier = pltpu.get_barrier_semaphore()
    peers = [mate(o) for o in range(1, TM)] + [to(g, (z + k) % nz, y) for k in range(1, nz)]
    for p in peers:
        pl.semaphore_signal(barrier, inc=1, device_id=p, device_id_type=MESH)
    pl.semaphore_wait(barrier, len(peers))

    def tabc(k, zt, zd, p):
        piece = tab.at[zt, pl.ds(p * BS, BS)]
        return copy(piece, piece, s_tab.at[k, p], r_tab.at[zt, p], to(g, zd, y))

    load_tab.wait()
    if cf.line:
        own_up = [tabc(0, z, z_mate, p) for p in range(per)]
        own_cross = [tabc(1, z, z_inner, p) for p in range(per)]
        f_mate = [tabc(2, z_mate, z_inner, p) for p in range(per)]
        f_inner = [tabc(3, z_inner, z_mate, p) for p in range(per)]
        f_edge = [tabc(4, z_edge, z_mate, p) for p in range(per)]
        for q in own_up:
            q.start()

        @pl.when(inner)
        def _():
            for q in own_cross:
                q.start()
    else:
        spread = [tabc(k, z, (z + k) % nz, p) for k in range(1, nz) for p in range(per)]
        for q in spread:
            q.start()

    def forward(kinds, p):
        if cf.line:

            @pl.when(inner)
            def _():
                for kind in kinds:
                    kind[p].wait_recv()
                    kind[p].start()

    b = block_row[...]
    hold, sub = b >> bits(cf.owned), b & (cf.owned - 1)
    zb, yb = hold >> bits(ny), hold & (ny - 1)
    gb, jb = sub >> bits(per), sub & (per - 1)
    ob = ((yb - y + ny) & (ny - 1)) * nx + (((gb >> 1) - x + nx) & (nx - 1))
    ob = ob * 2 + (((gb & 1) - c + 2) & 1)
    if cf.line:
        hb = zb >> 1
        qb = jnp.where(hb == half, jnp.where(zb == z, 3, 2), (zb + hb) & 1)
    else:
        qb = (zb - z - 1 + nz) & (nz - 1)
    place = ((qb >> bits(zs)) * TM + ob) * MSG + ((qb & (zs - 1)) * per + jb) * depth

    step = min(256, npts)
    before = (
        lax.broadcasted_iota(I32, (step, step), 0) < lax.broadcasted_iota(I32, (step, step), 1)
    ).astype(BF16)
    seen = jnp.zeros((cf.n_blocks, 1), F32)
    for t in range(npts // step):
        here = slice(t * step, (t + 1) * step)
        member = (lax.broadcasted_iota(I32, (cf.n_blocks, step), 0) == b[:, here]).astype(F32)
        prior = jnp.dot(member.astype(BF16), before, preferred_element_type=F32) + seen
        rank = jnp.sum(member * prior, axis=0, keepdims=True)
        seen = seen + jnp.sum(member, axis=1, keepdims=True)
        slot = place[:, here] + rank.astype(I32)
        slot_row[:, here] = slot
        slot_col[here, :] = jnp.transpose(jnp.broadcast_to(slot.astype(F32), (8, step)))
    want_row = jnp.broadcast_to((final_row[...] + 1).astype(F32), (8, npts)).astype(BF16)
    load_points.wait()

    pts_c = {
        (s, o): copy(out.at[s, o], recv.at[s, o], s_pts.at[s, o], r_pts.at[s, o], mate(o))
        for s in range(steps)
        for o in range(1, TM)
    }
    tgt_c = {
        (s, o): copy(tgt_out.at[s, o], tgt_in.at[s, o], s_tgt.at[s, o], r_tgt.at[s, o], mate(o))
        for s in range(steps)
        for o in range(1, TM)
    }
    ret_c = {
        (s, o): copy(
            dist.at[s, o],
            ret.at[s, o],
            s_ret.at[s, o],
            r_ret.at[s, o],
            to((x + nx - split(o)[1]) % nx * 2 + (c + split(o)[2]) % 2, z, (y + ny - split(o)[0]) % ny),
        )
        for s in range(steps)
        for o in range(1, TM)
    }

    def pack(s):
        for lo in list(range(TM - 2, -1, -2)):
            base = (s * TM + lo) * MSG
            hot = (lax.broadcasted_iota(I32, (2 * MSG, npts), 0) + base == slot_row[...]).astype(BF16)
            pts = jnp.dot(hot, points[...], preferred_element_type=F32).astype(BF16)
            tg = nt(want_row, hot)
            for i in range(2):
                o = lo + i
                rows, lanes = pts[i * MSG : (i + 1) * MSG], tg[:, i * MSG : (i + 1) * MSG]
                if o:
                    out[s, o] = rows
                    tgt_out[s, o] = lanes
                    tgt_c[s, o].start()
                    pts_c[s, o].start()
                else:
                    recv[s, 0] = rows
                    tgt_in[s, 0] = lanes

    def each(n, body):
        if n <= 2:
            for i in range(n):
                body(i)
        else:
            pl.loop(0, n)(body)

    ones = jnp.ones((8, R), BF16)

    def sums(s):
        for o in range(1, TM):
            tgt_c[s, o].wait_recv()
            pts_c[s, o].wait_recv()
        row = jnp.concatenate([tgt_in[s, o][0:1] for o in range(TM)], axis=1).astype(I32) - 1
        in_blk = (lax.broadcasted_iota(I32, (1, R), 1) & (MSG - 1)) >> bits(depth)

        def block(blk, own):
            want = jnp.where(in_blk == blk, row, -1)
            hot = (lax.broadcasted_iota(I32, (BS, R), 0) == want).astype(BF16)
            q, j = s * zs + blk // per, blk % per
            here = pl.ds(j * BS if isinstance(j, int) else pl.multiple_of(j * BS, BS), BS)
            cnt[q, j] = nt(ones, hot)
            total = jnp.dot(hot, recv[s].reshape(R, width), preferred_element_type=F32)
            if own:
                own_sum[here, :] = total
            else:
                part[q, here, :] = total.astype(BF16)

        n_own = per if s == steps - 1 else 0
        each(nblk - n_own, lambda blk: block(blk, False))
        for blk in range(nblk - n_own, nblk):
            block(blk, True)

    def dists(s):
        def block(blk):
            q, j = s * zs + blk // per, blk % per
            here = pl.ds(j * BS if isinstance(j, int) else pl.multiple_of(j * BS, BS), BS)
            rows = pl.ds(blk * depth if isinstance(blk, int) else pl.multiple_of(blk * depth, depth), depth)
            pts = recv[s, :, rows, :].reshape(TM * depth, width)
            table = tab[zq(q), here, :]
            cross = nt(pts, table)
            wide, twide = pts.astype(F32), table.astype(F32)
            rn = jnp.sum(wide * wide, axis=1, keepdims=True)
            cn = jnp.sum(twide * twide, axis=1, keepdims=True)
            cn = jnp.transpose(jnp.broadcast_to(cn, (BS, MSG)))[0:1]
            res = ((rn - 2.0 * cross + cn) / width).astype(BF16)
            dist[s, :, rows, :] = res.reshape(TM, depth, BS)

        each(nblk, block)
        for o in list(range(2, TM)) + [1]:
            ret_c[s, o].start()
        ret[s, 0] = dist[s, 0]

    gathered = []

    def gather(s):
        for o in range(1, TM):
            ret_c[s, o].wait_recv()
        first = not gathered
        gathered.append(s)
        ptile = min(256, npts)

        @pl.loop(0, npts // ptile)
        def _(t):
            here = pl.ds(pl.multiple_of(t * ptile, ptile), ptile)
            where = slot_col[here, 0:1].astype(I32)
            hot = (lax.broadcasted_iota(I32, (ptile, R), 1) + s * R == where).astype(BF16)
            acc = jnp.dot(hot, ret[s].reshape(R, BS), preferred_element_type=F32)
            if not first:
                acc += distances[here, :].astype(F32)
            distances[here, :] = acc.astype(BF16)

    if cf.line:
        to_agg = {
            q: [
                copy(part.at[q], agg_in.at[q], s_sum.at[q], r_agg.at[q], to(g, z_mate, y)),
                copy(cnt.at[q], cagg_in.at[q], s_cnt.at[q], r_cagg.at[q], to(g, z_mate, y)),
            ]
            for q in (0, 1)
        }
        to_far = {
            q: [
                copy(part.at[q], fin_in.at[1], s_sum.at[q], r_fin.at[1], to(g, order[q], y)),
                copy(cnt.at[q], cfin_in.at[1], s_cnt.at[q], r_cfin.at[1], to(g, order[q], y)),
            ]
            for q in (0, 1)
        }
        to_mate = [
            copy(part.at[2], fin_in.at[0], s_sum.at[2], r_fin.at[0], to(g, z_mate, y)),
            copy(cnt.at[2], cfin_in.at[0], s_cnt.at[2], r_cfin.at[0], to(g, z_mate, y)),
        ]
        finals = to_mate + to_far[0]

        def lift(q):
            @pl.when(edge)
            def _():
                for k in to_agg[q]:
                    k.start()

        def merge(q):
            @pl.when(inner)
            def _():
                for k in to_agg[q]:
                    k.wait_recv()

                @pl.loop(0, per)
                def _(j):
                    here = pl.ds(pl.multiple_of(j * BS, BS), BS)
                    both = part[q, here, :].astype(F32) + agg_in[q, here, :].astype(F32)
                    part[q, here, :] = both.astype(BF16)

                cnt[q] = cnt[q] + cagg_in[q]
                for k in to_far[q]:
                    k.start()

        def tables(q):
            @pl.when(edge)
            def _():
                for p in range(per):
                    tabc(3, order[q], z, p).wait_recv()

    else:
        direct = []
        for q in range(nz - 1):
            direct.append(copy(part.at[q], fin_in.at[q], s_sum.at[q], r_fin.at[q], to(g, zq(q), y)))
            direct.append(copy(cnt.at[q], cfin_in.at[q], s_cnt.at[q], r_cfin.at[q], to(g, zq(q), y)))
        finals = direct

    def group(k):
        dx, dc = k // 2, k % 2
        return (x + dx) % nx * 2 + (c + dc) % 2

    x_c = {k: copy(xs.at[group(k)], xin.at[k - 1], s_x.at[k], r_x.at[k], to(group(k), z, y)) for k in range(1, G)}

    def finish():
        for q in finals:
            q.wait_recv()
        for j in range(per):
            here = pl.ds(j * BS, BS)
            total, many = own_sum[here, :], cnt[nz - 1, j]
            for f in range(cf.fins):
                total += fin_in[f, here, :].astype(F32)
                many += cfin_in[f, j]
            many = 1.0 / (jnp.transpose(many)[:, 0:1] + 1.0)
            fresh = ((total + tab[z, here, :].astype(F32)) * many).astype(BF16)
            for k in range(G):
                xs[k, here, :] = fresh[:, k * share : (k + 1) * share]
        for k in list(range(2, G)) + [1]:
            x_c[k].start()

    def settle(gg, block):
        fresh_out[pl.ds(pl.multiple_of(gg * quarter, quarter), quarter), :] = block.astype(F32)

    if cf.line:
        pack(0)
        pack(1)
        pack(2)
        forward([f_mate, f_inner], 0)
        pack(3)
        for p in range(1, per):
            forward([f_mate, f_inner], p)
        sums(0)
        lift(0)
        for p in range(per):
            forward([f_edge], p)
        sums(1)
        lift(1)
        merge(0)
        tables(1)
        dists(1)
        sums(2)
        for k in to_mate:
            k.start()
        merge(1)
        tables(0)
        tables(2)
        dists(0)
        dists(2)
        sums(3)
        dists(3)
        finish()
        late = [1, 0, 2]
    else:
        for s in range(steps):
            pack(s)
        for s in range(steps):
            sums(s)
        for k in direct:
            k.start()
        for q in spread:
            q.wait_recv()
        for s in range(steps):
            dists(s)
        finish()
        late = list(range(steps - 1))
    for s in late:
        gather(s)
    settle(g, xs[g])
    for k in range(1, G):
        x_c[k].wait_recv()
        dx, dc = k // 2, k % 2
        settle((x + nx - dx) % nx * 2 + (c + dc) % 2, xin[k - 1])
    gather(steps - 1)

    for group_c in (pts_c, tgt_c, ret_c, x_c):
        for q in group_c.values():
            q.wait_send()
    if cf.line:
        for q in own_up + to_mate:
            q.wait_send()

        @pl.when(inner)
        def _():
            for q in own_cross + f_mate + f_inner + f_edge + to_far[0] + to_far[1]:
                q.wait_send()

        @pl.when(edge)
        def _():
            for q in to_agg[0] + to_agg[1]:
                q.wait_send()
    else:
        for q in spread + direct:
            q.wait_send()


def shards(points, blocks, finals, centroids):
    n_dev = lax.axis_size("dev")
    n_grp = lax.axis_size("grp")
    npts, width = points.shape
    rows = centroids.shape[0]
    cf = Sizes(n_grp, n_dev, npts, rows)
    share = width // n_grp
    quarter = cf.per * BS
    nz, tm, steps = cf.nz, cf.team, cf.steps

    dma = pltpu.SemaphoreType.DMA
    vm = pltpu.VMEM
    return pl.pallas_call(
        functools.partial(kernel, cf),
        out_shape=(
            jax.ShapeDtypeStruct((npts, BS), BF16),
            jax.ShapeDtypeStruct((rows, share), F32),
        ),
        in_specs=[pl.BlockSpec(memory_space=vm)] * 2 + [pl.BlockSpec(memory_space=pl.ANY)] * 2,
        out_specs=(pl.BlockSpec(memory_space=vm),) * 2,
        scratch_shapes=[
            vm((npts, width), BF16),
            vm((nz, quarter, width), BF16),
            vm((1, npts), I32),
            vm((npts, 8), F32),
            vm((steps, tm, MSG, width), BF16),
            vm((steps, tm, MSG, width), BF16),
            vm((steps, tm, 8, MSG), F32),
            vm((steps, tm, 8, MSG), F32),
            vm((nz - 1, quarter, width), BF16),
            vm((quarter, width), F32),
            vm((2, quarter, width), BF16),
            vm((cf.fins, quarter, width), BF16),
            vm((nz, cf.per, 8, BS), F32),
            vm((2, cf.per, 8, BS), F32),
            vm((cf.fins, cf.per, 8, BS), F32),
            vm((steps, tm, MSG, BS), BF16),
            vm((steps, tm, MSG, BS), BF16),
            vm((n_grp, quarter, share), BF16),
            vm((n_grp - 1, quarter, share), BF16),
            dma((steps, tm)), dma((steps, tm)), dma((steps, tm)), dma((steps, tm)),
            dma((max(5, nz), cf.per)), dma((nz, cf.per)),
            dma((nz - 1,)), dma((2,)), dma((cf.fins,)), dma((nz - 1,)), dma((2,)), dma((cf.fins,)),
            dma((steps, tm)), dma((steps, tm)), dma((n_grp,)), dma((n_grp,)), dma((2,)),
        ],
        compiler_params=pltpu.CompilerParams(
            collective_id=0, has_side_effects=True, vmem_limit_bytes=67_000_000
        ),
    )(blocks.reshape(1, npts), finals.reshape(1, npts), points, centroids)


def solution(mesh):
    placed = (P(("grp", "dev"), None), P(("grp", "dev"), None), P(("grp", "dev")), P("dev", None))
    return jax.shard_map(
        shards,
        mesh=mesh,
        in_specs=placed,
        out_specs=(P(("grp", "dev"), None), P("dev", "grp")),
        check_vma=False,
    )
```

```python
import functools

import jax
import jax.numpy as jnp
from jax import lax
from jax.experimental import pallas as pl
from jax.experimental.pallas import tpu as pltpu
from jax.sharding import PartitionSpec as P

BS = 256
MSG = 128
MESH = pl.DeviceIdType.MESH
F32, BF16, I32 = jnp.float32, jnp.bfloat16, jnp.int32


def bits(n):
    return n.bit_length() - 1


def nt(a, b):
    return lax.dot_general(a, b, (((1,), (1,)), ((), ())), preferred_element_type=F32)


class Sizes:
    def __init__(self, n_grp, n_dev, npts, rows):
        self.g, self.dev = n_grp, n_dev
        self.nx = n_grp // 2
        ny = 1
        while 8 * ny * ny <= n_dev:
            ny *= 2
        self.ny, self.nz = ny, n_dev // ny
        self.team = n_grp * ny
        self.owned = rows // BS
        self.per = self.owned // n_grp
        self.n_blocks = self.owned * n_dev
        self.depth = 2 * npts // self.n_blocks
        self.steps = self.nz * self.per * self.depth // MSG
        self.zs = self.nz // self.steps
        self.nblk = self.zs * self.per
        self.line = self.nz == 4
        self.fins = 2 if self.line else self.nz - 1


def kernel(
    cf,
    block_row, final_row, points_hbm, cent_hbm,
    distances, fresh_out,
    points, tab, slot_row, slot_col, out, recv, tgt_out, tgt_in,
    part, own_sum, agg_in, fin_in, cnt, cagg_in, cfin_in,
    dist, ret, xs, xin,
    s_pts, r_pts, s_tgt, r_tgt, s_tab, r_tab, s_sum, r_agg, r_fin, s_cnt, r_cagg, r_cfin,
    s_ret, r_ret, s_x, r_x, in_sem,
):
    G, nx, ny, nz, TM = cf.g, cf.nx, cf.ny, cf.nz, cf.team
    per, depth, steps, zs, nblk = cf.per, cf.depth, cf.steps, cf.zs, cf.nblk
    g, d = lax.axis_index("grp"), lax.axis_index("dev")
    x, c = g // 2, g % 2
    z, y = d // ny, d % ny
    npts, width = points.shape
    share = width // G
    quarter = per * BS
    R = TM * MSG

    def to(gg, zz, yy):
        return {"grp": gg, "dev": zz * ny + yy}

    def split(o):
        return o // (2 * nx), o // 2 % nx, o % 2

    def mate(o):
        dy, dx, dc = split(o)
        return to((x + dx) % nx * 2 + (c + dc) % 2, z, (y + dy) % ny)

    def copy(src, dst, ss, rs, dev):
        return pltpu.make_async_remote_copy(
            src_ref=src, dst_ref=dst, send_sem=ss, recv_sem=rs, device_id=dev, device_id_type=MESH
        )

    half = z // (nz // 2)
    if cf.line:
        z_mate, z_inner, z_edge = half * 2 + 1 - z % 2, 2 - half, 3 * (1 - half)
        inner = (z + half) % 2 == 1
        edge = (z + half) % 2 == 0
        order = [z_edge, z_inner, z_mate, z]

    def zq(q):
        return order[q] if cf.line else (z + q + 1) % nz

    load_tab = pltpu.make_async_copy(
        cent_hbm.at[pl.ds(pl.multiple_of(g * quarter, quarter), quarter)], tab.at[z], in_sem.at[0]
    )
    load_points = pltpu.make_async_copy(points_hbm, points, in_sem.at[1])
    load_tab.start()
    load_points.start()

    barrier = pltpu.get_barrier_semaphore()
    peers = [mate(o) for o in range(1, TM)] + [to(g, (z + k) % nz, y) for k in range(1, nz)]
    for p in peers:
        pl.semaphore_signal(barrier, inc=1, device_id=p, device_id_type=MESH)

    def tabc(k, zt, zd, p):
        piece = tab.at[zt, pl.ds(p * BS, BS)]
        return copy(piece, piece, s_tab.at[k, p], r_tab.at[zt, p], to(g, zd, y))

    def forward(kinds, p):
        if cf.line:

            @pl.when(inner)
            def _():
                for kind in kinds:
                    kind[p].wait_recv()
                    kind[p].start()

    b = block_row[...]
    hold, sub = b >> bits(cf.owned), b & (cf.owned - 1)
    zb, yb = hold >> bits(ny), hold & (ny - 1)
    gb, jb = sub >> bits(per), sub & (per - 1)
    ob = ((yb - y + ny) & (ny - 1)) * nx + (((gb >> 1) - x + nx) & (nx - 1))
    ob = ob * 2 + (((gb & 1) - c + 2) & 1)
    if cf.line:
        hb = zb >> 1
        qb = jnp.where(hb == half, jnp.where(zb == z, 3, 2), (zb + hb) & 1)
    else:
        qb = (zb - z - 1 + nz) & (nz - 1)
    place = ((qb >> bits(zs)) * TM + ob) * MSG + ((qb & (zs - 1)) * per + jb) * depth

    step = min(256, npts)
    before = (
        lax.broadcasted_iota(I32, (step, step), 0) < lax.broadcasted_iota(I32, (step, step), 1)
    ).astype(BF16)
    seen = jnp.zeros((cf.n_blocks, 1), F32)
    for t in range(npts // step):
        here = slice(t * step, (t + 1) * step)
        member = (lax.broadcasted_iota(I32, (cf.n_blocks, step), 0) == b[:, here]).astype(F32)
        prior = jnp.dot(member.astype(BF16), before, preferred_element_type=F32) + seen
        rank = jnp.sum(member * prior, axis=0, keepdims=True)
        seen = seen + jnp.sum(member, axis=1, keepdims=True)
        slot = place[:, here] + rank.astype(I32)
        slot_row[:, here] = slot
        slot_col[here, :] = jnp.transpose(jnp.broadcast_to(slot.astype(F32), (8, step)))
    want_row = jnp.broadcast_to((final_row[...] + 1).astype(F32), (8, npts)).astype(BF16)
    load_points.wait()

    pts_c = {
        (s, o): copy(out.at[s, o], recv.at[s, o], s_pts.at[s, o], r_pts.at[s, o], mate(o))
        for s in range(steps)
        for o in range(1, TM)
    }
    tgt_c = {
        (s, o): copy(tgt_out.at[s, o], tgt_in.at[s, o], s_tgt.at[s, o], r_tgt.at[s, o], mate(o))
        for s in range(steps)
        for o in range(1, TM)
    }
    ret_c = {
        (s, o): copy(
            dist.at[s, o],
            ret.at[s, o],
            s_ret.at[s, o],
            r_ret.at[s, o],
            to((x + nx - split(o)[1]) % nx * 2 + (c + split(o)[2]) % 2, z, (y + ny - split(o)[0]) % ny),
        )
        for s in range(steps)
        for o in range(1, TM)
    }

    def tile(s, lo):
        base = (s * TM + lo) * MSG
        hot = (lax.broadcasted_iota(I32, (2 * MSG, npts), 0) + base == slot_row[...]).astype(BF16)
        pts = jnp.dot(hot, points[...], preferred_element_type=F32).astype(BF16)
        tg = nt(want_row, hot)
        for i in range(2):
            o = lo + i
            rows, lanes = pts[i * MSG : (i + 1) * MSG], tg[:, i * MSG : (i + 1) * MSG]
            if o:
                out[s, o] = rows
                tgt_out[s, o] = lanes
            else:
                recv[s, 0] = rows
                tgt_in[s, 0] = lanes

    def send(s, lo):
        for o in (lo, lo + 1):
            if o:
                tgt_c[s, o].start()
                pts_c[s, o].start()

    def pack(s):
        for lo in range(TM - 2, -1, -2):
            if (s, lo) != (0, TM - 2):
                tile(s, lo)
                send(s, lo)

    tile(0, TM - 2)
    pl.semaphore_wait(barrier, len(peers))
    send(0, TM - 2)

    load_tab.wait()
    if cf.line:
        own_up = [tabc(0, z, z_mate, p) for p in range(per)]
        own_cross = [tabc(1, z, z_inner, p) for p in range(per)]
        f_mate = [tabc(2, z_mate, z_inner, p) for p in range(per)]
        f_inner = [tabc(3, z_inner, z_mate, p) for p in range(per)]
        f_edge = [tabc(4, z_edge, z_mate, p) for p in range(per)]
        for q in own_up:
            q.start()

        @pl.when(inner)
        def _():
            for q in own_cross:
                q.start()
    else:
        spread = [tabc(k, z, (z + k) % nz, p) for k in range(1, nz) for p in range(per)]
        for q in spread:
            q.start()

    def each(n, body):
        if n <= 2:
            for i in range(n):
                body(i)
        else:
            pl.loop(0, n)(body)

    ones = jnp.ones((8, R), BF16)

    def sums(s):
        for o in range(1, TM):
            tgt_c[s, o].wait_recv()
            pts_c[s, o].wait_recv()
        row = jnp.concatenate([tgt_in[s, o][0:1] for o in range(TM)], axis=1).astype(I32) - 1
        in_blk = (lax.broadcasted_iota(I32, (1, R), 1) & (MSG - 1)) >> bits(depth)

        def block(blk, own):
            want = jnp.where(in_blk == blk, row, -1)
            hot = (lax.broadcasted_iota(I32, (BS, R), 0) == want).astype(BF16)
            q, j = s * zs + blk // per, blk % per
            here = pl.ds(j * BS if isinstance(j, int) else pl.multiple_of(j * BS, BS), BS)
            cnt[q, j] = nt(ones, hot)
            total = jnp.dot(hot, recv[s].reshape(R, width), preferred_element_type=F32)
            if own:
                own_sum[here, :] = total
            else:
                part[q, here, :] = total.astype(BF16)

        n_own = per if s == steps - 1 else 0
        each(nblk - n_own, lambda blk: block(blk, False))
        for blk in range(nblk - n_own, nblk):
            block(blk, True)

    def dists(s):
        def block(blk):
            q, j = s * zs + blk // per, blk % per
            here = pl.ds(j * BS if isinstance(j, int) else pl.multiple_of(j * BS, BS), BS)
            rows = pl.ds(blk * depth if isinstance(blk, int) else pl.multiple_of(blk * depth, depth), depth)
            pts = recv[s, :, rows, :].reshape(TM * depth, width)
            table = tab[zq(q), here, :]
            cross = nt(pts, table)
            wide, twide = pts.astype(F32), table.astype(F32)
            rn = jnp.sum(wide * wide, axis=1, keepdims=True)
            cn = jnp.sum(twide * twide, axis=1, keepdims=True)
            cn = jnp.transpose(jnp.broadcast_to(cn, (BS, MSG)))[0:1]
            res = ((rn - 2.0 * cross + cn) / width).astype(BF16)
            dist[s, :, rows, :] = res.reshape(TM, depth, BS)

        each(nblk, block)
        for o in list(range(2, TM)) + [1]:
            ret_c[s, o].start()
        ret[s, 0] = dist[s, 0]

    gathered = []

    def gather(s):
        for o in range(1, TM):
            ret_c[s, o].wait_recv()
        first = not gathered
        gathered.append(s)
        ptile = min(256, npts)

        @pl.loop(0, npts // ptile)
        def _(t):
            here = pl.ds(pl.multiple_of(t * ptile, ptile), ptile)
            where = slot_col[here, 0:1].astype(I32)
            hot = (lax.broadcasted_iota(I32, (ptile, R), 1) + s * R == where).astype(BF16)
            acc = jnp.dot(hot, ret[s].reshape(R, BS), preferred_element_type=F32)
            if not first:
                acc += distances[here, :].astype(F32)
            distances[here, :] = acc.astype(BF16)

    if cf.line:

        def pair(q, dst, cdst, rs, crs, zd):
            return [
                copy(part.at[q], dst, s_sum.at[q], rs, to(g, zd, y)),
                copy(cnt.at[q], cdst, s_cnt.at[q], crs, to(g, zd, y)),
            ]

        def agg(q, k, zd):
            return pair(q, agg_in.at[k], cagg_in.at[k], r_agg.at[k], r_cagg.at[k], zd)

        def fin(q, k, zd):
            return pair(q, fin_in.at[k], cfin_in.at[k], r_fin.at[k], r_cfin.at[k], zd)

        edge_out = [agg(0, 0, z_mate), agg(1, 1, z_mate), fin(2, 0, z_mate)]
        inner_out = [agg(0, 2, z_inner), fin(1, 1, z_inner), fin(2, 0, z_mate)]
        inner_in = [agg(0, 0, z_mate), agg(1, 1, z_mate), agg(2, 2, z_inner)]

        def lift(q):
            @pl.when(edge)
            def _():
                for k in edge_out[q]:
                    k.start()

        def merge(q):
            @pl.when(inner)
            def _():
                for k in inner_in[q]:
                    k.wait_recv()

                @pl.loop(0, per)
                def _(j):
                    here = pl.ds(pl.multiple_of(j * BS, BS), BS)
                    both = part[q, here, :].astype(F32) + agg_in[q, here, :].astype(F32)
                    part[q, here, :] = both.astype(BF16)

                cnt[q] = cnt[q] + cagg_in[q]
                for k in inner_out[q]:
                    k.start()

        def tables(q):
            @pl.when(edge)
            def _():
                for p in range(per):
                    tabc(3, order[q], z, p).wait_recv()

        def arrive():
            for k in edge_out[2]:
                k.wait_recv()

            @pl.when(inner)
            def _():
                for k in inner_out[1]:
                    k.wait_recv()

                @pl.loop(0, per)
                def _(j):
                    here = pl.ds(pl.multiple_of(j * BS, BS), BS)
                    own_sum[here, :] += fin_in[1, here, :].astype(F32)

                cnt[nz - 1] = cnt[nz - 1] + cfin_in[1]

    else:
        direct = []
        for q in range(nz - 1):
            direct.append(copy(part.at[q], fin_in.at[q], s_sum.at[q], r_fin.at[q], to(g, zq(q), y)))
            direct.append(copy(cnt.at[q], cfin_in.at[q], s_cnt.at[q], r_cfin.at[q], to(g, zq(q), y)))

        def arrive():
            for q in direct:
                q.wait_recv()

    def group(k):
        dx, dc = k // 2, k % 2
        return (x + dx) % nx * 2 + (c + dc) % 2

    x_c = {k: copy(xs.at[group(k)], xin.at[k - 1], s_x.at[k], r_x.at[k], to(group(k), z, y)) for k in range(1, G)}

    def finish():
        arrive()
        for j in range(per):
            here = pl.ds(j * BS, BS)
            total, many = own_sum[here, :], cnt[nz - 1, j]
            for f in range(1 if cf.line else cf.fins):
                total += fin_in[f, here, :].astype(F32)
                many += cfin_in[f, j]
            many = 1.0 / (jnp.transpose(many)[:, 0:1] + 1.0)
            fresh = ((total + tab[z, here, :].astype(F32)) * many).astype(BF16)
            for k in range(G):
                xs[k, here, :] = fresh[:, k * share : (k + 1) * share]
        for k in list(range(2, G)) + [1]:
            x_c[k].start()

    def settle(gg, block):
        fresh_out[pl.ds(pl.multiple_of(gg * quarter, quarter), quarter), :] = block.astype(F32)

    if cf.line:
        pack(0)
        pack(1)
        pack(2)
        forward([f_mate, f_inner], 0)
        pack(3)
        for p in range(1, per):
            forward([f_mate, f_inner], p)
        sums(0)
        lift(0)
        for p in range(per):
            forward([f_edge], p)
        sums(1)
        lift(1)
        merge(0)
        tables(1)
        dists(1)
        sums(2)
        lift(2)
        merge(1)
        merge(2)
        tables(0)
        tables(2)
        dists(0)
        dists(2)
        sums(3)
        dists(3)
        finish()
        late = [1, 0, 2]
    else:
        for s in range(steps):
            pack(s)
        for s in range(steps):
            sums(s)
        for k in direct:
            k.start()
        for q in spread:
            q.wait_recv()
        for s in range(steps):
            dists(s)
        finish()
        late = list(range(steps - 1))
    for s in late + [steps - 1]:
        gather(s)
    settle(g, xs[g])
    for k in range(1, G):
        x_c[k].wait_recv()
        dx, dc = k // 2, k % 2
        settle((x + nx - dx) % nx * 2 + (c + dc) % 2, xin[k - 1])

    for group_c in (pts_c, tgt_c, ret_c, x_c):
        for q in group_c.values():
            q.wait_send()
    if cf.line:
        for q in own_up + edge_out[0] + edge_out[1] + edge_out[2]:
            q.wait_send()

        @pl.when(inner)
        def _():
            for q in own_cross + f_mate + f_inner + f_edge:
                q.wait_send()
    else:
        for q in spread + direct:
            q.wait_send()


def shards(points, blocks, finals, centroids):
    n_dev = lax.axis_size("dev")
    n_grp = lax.axis_size("grp")
    npts, width = points.shape
    rows = centroids.shape[0]
    cf = Sizes(n_grp, n_dev, npts, rows)
    share = width // n_grp
    quarter = cf.per * BS
    nz, tm, steps = cf.nz, cf.team, cf.steps

    dma = pltpu.SemaphoreType.DMA
    vm = pltpu.VMEM
    return pl.pallas_call(
        functools.partial(kernel, cf),
        out_shape=(vm((npts, BS), BF16), vm((rows, share), F32)),
        in_specs=[pl.BlockSpec(memory_space=vm)] * 2 + [pl.BlockSpec(memory_space=pl.ANY)] * 2,
        out_specs=(pl.BlockSpec(memory_space=vm),) * 2,
        scratch_shapes=[
            vm((npts, width), BF16),
            vm((nz, quarter, width), BF16),
            vm((1, npts), I32),
            vm((npts, 8), F32),
            vm((steps, tm, MSG, width), BF16),
            vm((steps, tm, MSG, width), BF16),
            vm((steps, tm, 8, MSG), F32),
            vm((steps, tm, 8, MSG), F32),
            vm((nz - 1, quarter, width), BF16),
            vm((quarter, width), F32),
            vm((3, quarter, width), BF16),
            vm((cf.fins, quarter, width), BF16),
            vm((nz, cf.per, 8, BS), F32),
            vm((3, cf.per, 8, BS), F32),
            vm((cf.fins, cf.per, 8, BS), F32),
            vm((steps, tm, MSG, BS), BF16),
            vm((steps, tm, MSG, BS), BF16),
            vm((n_grp, quarter, share), BF16),
            vm((n_grp - 1, quarter, share), BF16),
            dma((steps, tm)), dma((steps, tm)), dma((steps, tm)), dma((steps, tm)),
            dma((max(5, nz), cf.per)), dma((nz, cf.per)),
            dma((nz - 1,)), dma((3,)), dma((cf.fins,)), dma((nz - 1,)), dma((3,)), dma((cf.fins,)),
            dma((steps, tm)), dma((steps, tm)), dma((n_grp,)), dma((n_grp,)), dma((2,)),
        ],
        compiler_params=pltpu.CompilerParams(
            collective_id=0, has_side_effects=True, vmem_limit_bytes=58_000_000
        ),
    )(blocks.reshape(1, npts), finals.reshape(1, npts), points, centroids)


def solution(mesh):
    placed = (P(("grp", "dev"), None), P(("grp", "dev"), None), P(("grp", "dev")), P("dev", None))
    return jax.shard_map(
        shards,
        mesh=mesh,
        in_specs=placed,
        out_specs=(P(("grp", "dev"), None), P("dev", "grp")),
        check_vma=False,
    )
```

```python
import functools

import jax
import jax.numpy as jnp
from jax import lax
from jax.experimental import pallas as pl
from jax.experimental.pallas import tpu as pltpu
from jax.sharding import PartitionSpec as P

BS = 256
MSG = 128
MESH = pl.DeviceIdType.MESH
F32, BF16, I32 = jnp.float32, jnp.bfloat16, jnp.int32


def bits(n):
    return n.bit_length() - 1


def nt(a, b):
    return lax.dot_general(a, b, (((1,), (1,)), ((), ())), preferred_element_type=F32)


class Sizes:
    def __init__(self, n_grp, n_dev, npts, rows):
        self.g, self.dev = n_grp, n_dev
        self.nx = n_grp // 2
        ny = 1
        while 8 * ny * ny <= n_dev:
            ny *= 2
        self.ny, self.nz = ny, n_dev // ny
        self.team = n_grp * ny
        self.owned = rows // BS
        self.per = self.owned // n_grp
        self.n_blocks = self.owned * n_dev
        self.depth = 2 * npts // self.n_blocks
        self.steps = self.nz * self.per * self.depth // MSG
        self.zs = self.nz // self.steps
        self.nblk = self.zs * self.per
        self.line = self.nz == 4 and self.nx == 2
        self.fins = 2 if self.line else self.nz - 1


def kernel(
    cf,
    block_row, final_row, points_hbm, cent_hbm,
    distances, fresh_out,
    points, tab, slot_row, slot_col, out, recv, tgt_out, tgt_in,
    part, own_sum, agg_in, fin_in, cnt, cagg_in, cfin_in,
    dist, ret, xs, xin, tab_x, oth_sum, cnt_oth, x_out, x_in, cx_in,
    s_pts, r_pts, s_tgt, r_tgt, s_tab, r_tab, s_sum, r_agg, r_fin, s_cnt, r_cagg, r_cfin,
    s_ret, r_ret, s_x, r_x, s_side, r_side, s_cside, r_cside, in_sem,
):
    G, nx, ny, nz, TM = cf.g, cf.nx, cf.ny, cf.nz, cf.team
    per, depth, steps, zs, nblk = cf.per, cf.depth, cf.steps, cf.zs, cf.nblk
    g, d = lax.axis_index("grp"), lax.axis_index("dev")
    x, c = g // 2, g % 2
    z, y = d // ny, d % ny
    npts, width = points.shape
    share = width // G
    quarter = per * BS
    R = TM * MSG

    def to(gg, zz, yy):
        return {"grp": gg, "dev": zz * ny + yy}

    def split(o):
        return o // (2 * nx), o // 2 % nx, o % 2

    def near(s):
        return cf.line and s == steps - 1

    def mate(o, s=0):
        dy, dx, dc = split(o)
        return to((x + (0 if near(s) else dx)) % nx * 2 + (c + dc) % 2, z, (y + dy) % ny)

    def back(o, s):
        dy, dx, dc = split(o)
        return to((x + nx - (0 if near(s) else dx)) % nx * 2 + (c + dc) % 2, z, (y + ny - dy) % ny)

    def remote(s):
        return [o for o in range(TM) if (split(o)[0] or split(o)[2] if near(s) else o)]

    def start_of(xq, cq):
        return pl.multiple_of((cq * nx + xq) * quarter, quarter)

    def copy(src, dst, ss, rs, dev):
        return pltpu.make_async_remote_copy(
            src_ref=src, dst_ref=dst, send_sem=ss, recv_sem=rs, device_id=dev, device_id_type=MESH
        )

    half = z // (nz // 2)
    if cf.line:
        z_mate, z_inner, z_edge = half * 2 + 1 - z % 2, 2 - half, 3 * (1 - half)
        mid = (z + half) % 2
        inner = mid == 1
        edge = mid == 0
        order = [z_edge, mid * z_mate + (1 - mid) * z_inner, mid * z_inner + (1 - mid) * z_mate, z]

    def zq(q):
        return order[q] if cf.line else (z + q + 1) % nz

    load_tab = pltpu.make_async_copy(
        cent_hbm.at[pl.ds(start_of(x, c), quarter)], tab.at[z], in_sem.at[0]
    )
    load_points = pltpu.make_async_copy(points_hbm, points, in_sem.at[1])
    load_points.start()
    load_tab.start()
    if cf.line:
        load_other = pltpu.make_async_copy(
            cent_hbm.at[pl.ds(start_of(1 - x, c), quarter)], tab_x, in_sem.at[2]
        )
        load_other.start()

    barrier = pltpu.get_barrier_semaphore()
    peers = [mate(o) for o in range(1, TM)] + [to(g, (z + k) % nz, y) for k in range(1, nz)]
    for p in peers:
        pl.semaphore_signal(barrier, inc=1, device_id=p, device_id_type=MESH)

    def tabc(k, zt, zd, p):
        piece = tab.at[zt, pl.ds(p * BS, BS)]
        return copy(piece, piece, s_tab.at[k, p], r_tab.at[zt, p], to(g, zd, y))

    def forward(kinds, p):
        if cf.line:

            @pl.when(inner)
            def _():
                for kind in kinds:
                    kind[p].wait_recv()
                    kind[p].start()

    b = block_row[...]
    hold, sub = b >> bits(cf.owned), b & (cf.owned - 1)
    zb, yb = hold >> bits(ny), hold & (ny - 1)
    gb, jb = sub >> bits(per), sub & (per - 1)
    ob = ((yb - y + ny) & (ny - 1)) * nx + (((gb & (nx - 1)) - x + nx) & (nx - 1))
    ob = ob * 2 + (((gb >> bits(nx)) - c + 2) & 1)
    if cf.line:
        hb = zb >> 1
        qb = jnp.where(hb == half, jnp.where(zb == z, 3, 2 - mid), ((zb + hb) & 1) * (1 + mid))
    else:
        qb = (zb - z - 1 + nz) & (nz - 1)
    place = ((qb >> bits(zs)) * TM + ob) * MSG + ((qb & (zs - 1)) * per + jb) * depth

    step = min(256, npts)
    before = (
        lax.broadcasted_iota(I32, (step, step), 0) < lax.broadcasted_iota(I32, (step, step), 1)
    ).astype(BF16)
    seen = jnp.zeros((cf.n_blocks, 1), F32)
    for t in range(npts // step):
        here = slice(t * step, (t + 1) * step)
        member = (lax.broadcasted_iota(I32, (cf.n_blocks, step), 0) == b[:, here]).astype(F32)
        prior = jnp.dot(member.astype(BF16), before, preferred_element_type=F32) + seen
        rank = jnp.sum(member * prior, axis=0, keepdims=True)
        seen = seen + jnp.sum(member, axis=1, keepdims=True)
        slot = place[:, here] + rank.astype(I32)
        slot_row[:, here] = slot
        slot_col[here, :] = jnp.transpose(jnp.broadcast_to(slot.astype(F32), (8, step)))
    want_row = jnp.broadcast_to((final_row[...] + 1).astype(F32), (8, npts)).astype(BF16)
    load_points.wait()

    pts_c, tgt_c, ret_c = {}, {}, {}
    for s in range(steps):
        for o in remote(s):
            pts_c[s, o] = copy(out.at[s, o], recv.at[s, o], s_pts.at[s, o], r_pts.at[s, o], mate(o, s))
            tgt_c[s, o] = copy(tgt_out.at[s, o], tgt_in.at[s, o], s_tgt.at[s, o], r_tgt.at[s, o], mate(o, s))
            ret_c[s, o] = copy(dist.at[s, o], ret.at[s, o], s_ret.at[s, o], r_ret.at[s, o], back(o, s))

    def tile(s, lo):
        base = (s * TM + lo) * MSG
        hot = (lax.broadcasted_iota(I32, (2 * MSG, npts), 0) + base == slot_row[...]).astype(BF16)
        pts = jnp.dot(hot, points[...], preferred_element_type=F32).astype(BF16)
        tg = nt(want_row, hot)
        for i in range(2):
            o = lo + i
            rows, lanes = pts[i * MSG : (i + 1) * MSG], tg[:, i * MSG : (i + 1) * MSG]
            if o in remote(s):
                out[s, o] = rows
                tgt_out[s, o] = lanes
            else:
                recv[s, o] = rows
                tgt_in[s, o] = lanes

    def send(s, lo):
        for o in (lo, lo + 1):
            if o in remote(s):
                tgt_c[s, o].start()
                pts_c[s, o].start()

    def pack(s):
        for lo in range(TM - 2, -1, -2):
            if (s, lo) != (0, TM - 2):
                tile(s, lo)
                send(s, lo)

    tile(0, TM - 2)
    pl.semaphore_wait(barrier, len(peers))
    send(0, TM - 2)

    load_tab.wait()
    if cf.line:
        own_up = [tabc(0, z, z_mate, p) for p in range(per)]
        own_cross = [tabc(1, z, z_inner, p) for p in range(per)]
        f_mate = [tabc(2, z_mate, z_inner, p) for p in range(per)]
        f_inner = [tabc(3, z_inner, z_mate, p) for p in range(per)]
        f_edge = [tabc(4, z_edge, z_mate, p) for p in range(per)]
        for q in own_up:
            q.start()

        @pl.when(inner)
        def _():
            for q in own_cross:
                q.start()
    else:
        spread = [tabc(k, z, (z + k) % nz, p) for k in range(1, nz) for p in range(per)]
        for q in spread:
            q.start()

    def each(n, body):
        if n <= 2:
            for i in range(n):
                body(i)
        else:
            pl.loop(0, n)(body)

    ones = jnp.ones((8, R), BF16)

    def sums(s):
        for o in range(1, TM):
            tgt_c[s, o].wait_recv()
            pts_c[s, o].wait_recv()
        row = jnp.concatenate([tgt_in[s, o][0:1] for o in range(TM)], axis=1).astype(I32) - 1
        in_blk = (lax.broadcasted_iota(I32, (1, R), 1) & (MSG - 1)) >> bits(depth)

        def block(blk, own):
            want = jnp.where(in_blk == blk, row, -1)
            hot = (lax.broadcasted_iota(I32, (BS, R), 0) == want).astype(BF16)
            q, j = s * zs + blk // per, blk % per
            here = pl.ds(j * BS if isinstance(j, int) else pl.multiple_of(j * BS, BS), BS)
            cnt[q, j] = nt(ones, hot)
            total = jnp.dot(hot, recv[s].reshape(R, width), preferred_element_type=F32)
            if own:
                own_sum[here, :] = total
            else:
                part[q, here, :] = total.astype(BF16)

        n_own = per if s == steps - 1 else 0
        each(nblk - n_own, lambda blk: block(blk, False))
        for blk in range(nblk - n_own, nblk):
            block(blk, True)

    def distance(pts, table):
        cross = nt(pts, table)
        wide, twide = pts.astype(F32), table.astype(F32)
        rn = jnp.sum(wide * wide, axis=1, keepdims=True)
        cn = jnp.sum(twide * twide, axis=1, keepdims=True)
        cn = jnp.transpose(jnp.broadcast_to(cn, (BS, MSG)))[0:1]
        return ((rn - 2.0 * cross + cn) / width).astype(BF16)

    def give(s, units):
        far = remote(s)
        for o in [o for o in units if o in far]:
            ret_c[s, o].start()
        for o in units:
            if o not in far:
                ret[s, o] = dist[s, o]

    def dists(s):
        def block(blk):
            q, j = s * zs + blk // per, blk % per
            here = pl.ds(j * BS if isinstance(j, int) else pl.multiple_of(j * BS, BS), BS)
            rows = pl.ds(blk * depth if isinstance(blk, int) else pl.multiple_of(blk * depth, depth), depth)
            pts = recv[s, :, rows, :].reshape(TM * depth, width)
            dist[s, :, rows, :] = distance(pts, tab[zq(q), here, :]).reshape(TM, depth, BS)

        each(nblk, block)
        give(s, list(range(2, TM)) + [0, 1])

    def both(ref, s, dx, *rest):
        return jnp.concatenate([ref[(s, slice(u, u + 2)) + rest] for u in range(dx * 2, TM, 2 * nx)], axis=0)

    def near_sums(s, dx):
        units = [u + dc for u in range(dx * 2, TM, 2 * nx) for dc in range(2)]
        for o in units:
            if o in remote(s):
                tgt_c[s, o].wait_recv()
                pts_c[s, o].wait_recv()
        n = len(units) * MSG
        row = jnp.concatenate([tgt_in[s, o][0:1] for o in units], axis=1).astype(I32) - 1
        in_blk = (lax.broadcasted_iota(I32, (1, n), 1) & (MSG - 1)) >> bits(depth)
        for j in range(per):
            want = jnp.where(in_blk == j, row, -1)
            hot = (lax.broadcasted_iota(I32, (BS, n), 0) == want).astype(BF16)
            many = nt(jnp.ones((8, n), BF16), hot)
            total = jnp.dot(hot, both(recv, s, dx).reshape(n, width), preferred_element_type=F32)
            if dx:
                cnt_oth[j] = many
                oth_sum[j * BS : (j + 1) * BS, :] = total
            else:
                cnt[nz - 1, j] = many
                own_sum[j * BS : (j + 1) * BS, :] = total

    def near_dists(s, dx):
        for j in range(per):
            here, rows = slice(j * BS, (j + 1) * BS), slice(j * depth, (j + 1) * depth)
            pts = both(recv, s, dx, rows).reshape(-1, width)
            table = tab_x[here, :] if dx else tab[z, here, :]
            res = distance(pts, table).reshape(-1, depth, BS)
            for i, u in enumerate(range(dx * 2, TM, 2 * nx)):
                dist[s, u : u + 2, rows, :] = res[2 * i : 2 * i + 2]
        give(s, [u + dc for u in range(dx * 2, TM, 2 * nx) for dc in range(2)])

    gathered = []

    def gather(s, lo, hi):
        for o in remote(s):
            if lo <= o < hi:
                ret_c[s, o].wait_recv()
        first = not gathered
        gathered.append(s)
        ptile = min(256, npts)
        n = (hi - lo) * MSG

        @pl.loop(0, npts // ptile, unroll=2)
        def _(t):
            here = pl.ds(pl.multiple_of(t * ptile, ptile), ptile)
            where = slot_col[here, 0:1].astype(I32)
            hot = (lax.broadcasted_iota(I32, (ptile, n), 1) + s * R + lo * MSG == where).astype(BF16)
            acc = jnp.dot(hot, ret[s, lo:hi].reshape(n, BS), preferred_element_type=F32)
            if not first:
                acc += distances[here, :].astype(F32)
            distances[here, :] = acc.astype(BF16)

    if cf.line:

        def pair(q, j, dst, cdst, rs, crs, zd):
            piece = pl.ds(j * BS, BS)
            return [
                copy(part.at[q, piece], dst.at[piece], s_sum.at[q, j], rs.at[j], to(g, zd, y)),
                copy(cnt.at[q, j], cdst.at[j], s_cnt.at[q, j], crs.at[j], to(g, zd, y)),
            ]

        def agg(q, j, k, zd):
            return pair(q, j, agg_in.at[k], cagg_in.at[k], r_agg.at[k], r_cagg.at[k], zd)

        def fin(q, j, k, zd):
            return pair(q, j, fin_in.at[k], cfin_in.at[k], r_fin.at[k], r_cfin.at[k], zd)

        edge_out, inner_out, inner_in = {}, {}, {}
        for j in range(per):
            edge_out[0, j], edge_out[1, j], edge_out[2, j] = agg(0, j, 0, z_mate), agg(1, j, 1, z_mate), fin(2, j, 0, z_mate)
            inner_out[0, j], inner_out[1, j], inner_out[2, j] = (
                agg(0, j, 2, z_inner), fin(1, j, 0, z_mate), fin(2, j, 1, z_inner)
            )
            inner_in[0, j], inner_in[1, j], inner_in[2, j] = agg(0, j, 0, z_mate), agg(1, j, 2, z_inner), agg(2, j, 1, z_mate)
        slot_of = [0, 2, 1]

        def lift(q):
            @pl.when(edge)
            def _():
                for j in range(per):
                    for k in edge_out[q, j]:
                        k.start()

        def merge(q, j):
            @pl.when(inner)
            def _():
                for k in inner_in[q, j]:
                    k.wait_recv()
                here = pl.ds(j * BS, BS)
                total = part[q, here, :].astype(F32) + agg_in[slot_of[q], here, :].astype(F32)
                part[q, here, :] = total.astype(BF16)
                cnt[q, j] = cnt[q, j] + cagg_in[slot_of[q], j]
                for k in inner_out[q, j]:
                    k.start()

        def tables(q):
            @pl.when(edge)
            def _():
                for p in range(per):
                    tabc(3, order[q], z, p).wait_recv()

        def arrive():
            for j in range(per):
                here = pl.ds(j * BS, BS)
                for k in edge_out[2, j]:
                    k.wait_recv()
                own_sum[here, :] += fin_in[0, here, :].astype(F32)
                cnt[nz - 1, j] = cnt[nz - 1, j] + cfin_in[0, j]

            @pl.when(inner)
            def _():
                for j in range(per):
                    here = pl.ds(j * BS, BS)
                    for k in inner_out[2, j]:
                        k.wait_recv()
                    own_sum[here, :] += fin_in[1, here, :].astype(F32)
                    cnt[nz - 1, j] = cnt[nz - 1, j] + cfin_in[1, j]

    else:
        direct = []
        for q in range(nz - 1):
            direct.append(copy(part.at[q], fin_in.at[q], s_sum.at[q, 0], r_fin.at[q, 0], to(g, zq(q), y)))
            direct.append(copy(cnt.at[q], cfin_in.at[q], s_cnt.at[q, 0], r_cfin.at[q, 0], to(g, zq(q), y)))

        def arrive():
            for q in direct:
                q.wait_recv()

    def group(k):
        dx, dc = k // 2, k % 2
        return (x + dx) % nx * 2 + (c + dc) % 2

    def settle(xq, cq, block):
        fresh_out[pl.ds(start_of(xq, cq), quarter), :] = block.astype(F32)

    if cf.line:
        side = 2 * share
        mine, theirs = (pl.ds(pl.multiple_of(k * side, side), side) for k in (x, 1 - x))
        across, beside = to((1 - x) * 2 + c, z, y), to(x * 2 + 1 - c, z, y)
        side_c = [
            [
                [
                    copy(x_out.at[k, j], x_in.at[k, j], s_side.at[k, j], r_side.at[k, j], across),
                    copy((cnt_oth if k else cnt.at[nz - 1]).at[j], cx_in.at[k, j], s_cside.at[k, j], r_cside.at[k, j], across),
                ]
                for j in range(per)
            ]
            for k in (0, 1)
        ]
        x_c = {k: copy(xs.at[(1 - c) * 2 + k], xin.at[k], s_x.at[k], r_x.at[k], beside) for k in (0, 1)}

        def cross(k):
            total = oth_sum if k else own_sum
            for j in range(per):
                here = pl.ds(j * BS, BS)
                x_out[k, j] = total[here, theirs].astype(BF16)
                for q in side_c[k][j]:
                    q.start()

        def finish(k):
            for j in range(per):
                for q in side_c[1 - k][j]:
                    q.wait_recv()
                here = pl.ds(j * BS, BS)
                total = oth_sum[here, mine] if k else own_sum[here, mine]
                old = tab_x[here, mine] if k else tab[z, here, mine]
                many = (cnt_oth[j] if k else cnt[nz - 1, j]) + cx_in[1 - k, j]
                many = 1.0 / (jnp.transpose(many)[:, 0:1] + 1.0)
                total = total + x_in[1 - k, j].astype(F32) + old.astype(F32)
                fresh = (total * many).astype(BF16)
                for i in range(2):
                    xs[i * 2 + k, here, :] = fresh[:, i * share : (i + 1) * share]
            x_c[k].start()
            settle((x + k) % 2, c, xs[c * 2 + k])

    else:
        x_c = {k: copy(xs.at[group(k)], xin.at[k - 1], s_x.at[k], r_x.at[k], to(group(k), z, y)) for k in range(1, G)}

        def finish():
            arrive()
            for j in range(per):
                here = pl.ds(j * BS, BS)
                total, many = own_sum[here, :], cnt[nz - 1, j]
                for f in range(cf.fins):
                    total += fin_in[f, here, :].astype(F32)
                    many += cfin_in[f, j]
                many = 1.0 / (jnp.transpose(many)[:, 0:1] + 1.0)
                fresh = ((total + tab[z, here, :].astype(F32)) * many).astype(BF16)
                for k in range(G):
                    xs[k, here, :] = fresh[:, k * share : (k + 1) * share]
            for k in list(range(2, G)) + [1]:
                x_c[k].start()

    if cf.line:
        pack(0)
        pack(1)
        pack(2)
        forward([f_mate, f_inner], 0)
        pack(3)
        for p in range(1, per):
            forward([f_mate, f_inner], p)
        sums(0)
        lift(0)
        for p in range(per):
            forward([f_edge], p)
        sums(1)
        lift(1)
        for j in range(per):
            merge(0, j)
        tables(1)
        dists(1)
        merge(1, 0)
        sums(2)
        lift(2)
        for j in range(1, per):
            merge(1, j)
        for j in range(per):
            merge(2, j)
        tables(0)
        tables(2)
        dists(0)
        dists(2)
        load_other.wait()
        near_sums(3, 1)
        cross(1)
        near_dists(3, 1)
        gather(1, 0, TM // 2)
        gather(0, 0, TM // 2)
        gather(2, 0, TM // 2)
        near_sums(3, 0)
        arrive()
        cross(0)
        near_dists(3, 0)
        gather(1, TM // 2, TM)
        finish(0)
        gather(0, TM // 2, TM)
        gather(3, 0, TM // 2)
        gather(2, TM // 2, TM)
        finish(1)
        gather(3, TM // 2, TM)
        for k in (0, 1):
            x_c[k].wait_recv()
            settle((x + k) % 2, 1 - c, xin[k])
    else:
        for s in range(steps):
            pack(s)
        for s in range(steps):
            sums(s)
        for k in direct:
            k.start()
        for q in spread:
            q.wait_recv()
        for s in range(steps):
            dists(s)
        finish()
        for s in range(steps):
            gather(s, 0, TM)
        settle(x, c, xs[g])
        for k in range(1, G):
            x_c[k].wait_recv()
            dx, dc = k // 2, k % 2
            settle((x + nx - dx) % nx, (c + dc) % 2, xin[k - 1])

    for group_c in (pts_c, tgt_c, ret_c, x_c):
        for q in group_c.values():
            q.wait_send()
    if cf.line:
        for q in own_up:
            q.wait_send()
        for group_c in side_c[0] + side_c[1] + list(edge_out.values()):
            for q in group_c:
                q.wait_send()

        @pl.when(inner)
        def _():
            for q in own_cross + f_mate + f_inner + f_edge:
                q.wait_send()
    else:
        for q in spread + direct:
            q.wait_send()


def shards(points, blocks, finals, centroids):
    n_dev = lax.axis_size("dev")
    n_grp = lax.axis_size("grp")
    npts, width = points.shape
    rows = centroids.shape[0]
    cf = Sizes(n_grp, n_dev, npts, rows)
    share = width // n_grp
    quarter = cf.per * BS
    nz, tm, steps = cf.nz, cf.team, cf.steps

    dma = pltpu.SemaphoreType.DMA
    vm = pltpu.VMEM
    return pl.pallas_call(
        functools.partial(kernel, cf),
        out_shape=(vm((npts, BS), BF16), vm((rows, share), F32)),
        in_specs=[pl.BlockSpec(memory_space=vm)] * 2 + [pl.BlockSpec(memory_space=pl.ANY)] * 2,
        out_specs=(pl.BlockSpec(memory_space=vm),) * 2,
        scratch_shapes=[
            vm((npts, width), BF16),
            vm((nz, quarter, width), BF16),
            vm((1, npts), I32),
            vm((npts, 8), F32),
            vm((steps, tm, MSG, width), BF16),
            vm((steps, tm, MSG, width), BF16),
            vm((steps, tm, 8, MSG), F32),
            vm((steps, tm, 8, MSG), F32),
            vm((nz - 1, quarter, width), BF16),
            vm((quarter, width), F32),
            vm((3, quarter, width), BF16),
            vm((cf.fins, quarter, width), BF16),
            vm((nz, cf.per, 8, BS), F32),
            vm((3, cf.per, 8, BS), F32),
            vm((cf.fins, cf.per, 8, BS), F32),
            vm((steps, tm, MSG, BS), BF16),
            vm((steps, tm, MSG, BS), BF16),
            vm((n_grp, quarter, share), BF16),
            vm((n_grp - 1, quarter, share), BF16),
            vm((quarter, width), BF16),
            vm((quarter, width), F32),
            vm((cf.per, 8, BS), F32),
            vm((2, cf.per, BS, 2 * share), BF16),
            vm((2, cf.per, BS, 2 * share), BF16),
            vm((2, cf.per, 8, BS), F32),
            dma((steps, tm)), dma((steps, tm)), dma((steps, tm)), dma((steps, tm)),
            dma((max(5, nz), cf.per)), dma((nz, cf.per)),
            dma((nz - 1, cf.per)), dma((3, cf.per)), dma((cf.fins, cf.per)), dma((nz - 1, cf.per)), dma((3, cf.per)), dma((cf.fins, cf.per)),
            dma((steps, tm)), dma((steps, tm)), dma((n_grp,)), dma((n_grp,)),
            dma((2, cf.per)), dma((2, cf.per)), dma((2, cf.per)), dma((2, cf.per)), dma((3,)),
        ],
        compiler_params=pltpu.CompilerParams(
            collective_id=0, has_side_effects=True, vmem_limit_bytes=58_000_000
        ),
    )(blocks.reshape(1, npts), finals.reshape(1, npts), points, centroids)


def solution(mesh):
    placed = (P(("grp", "dev"), None), P(("grp", "dev"), None), P(("grp", "dev")), P("dev", None))
    return jax.shard_map(
        shards,
        mesh=mesh,
        in_specs=placed,
        out_specs=(P(("grp", "dev"), None), P("dev", "grp")),
        check_vma=False,
    )
```

```python
import functools

import jax
import jax.numpy as jnp
from jax import lax
from jax.experimental import pallas as pl
from jax.experimental.pallas import tpu as pltpu
from jax.sharding import PartitionSpec as P

BS = 256
MSG = 128
MESH = pl.DeviceIdType.MESH
F32, BF16, I32 = jnp.float32, jnp.bfloat16, jnp.int32


def bits(n):
    return n.bit_length() - 1


def nt(a, b):
    return lax.dot_general(a, b, (((1,), (1,)), ((), ())), preferred_element_type=F32)


class Sizes:
    def __init__(self, n_grp, n_dev, npts, rows):
        self.g, self.dev = n_grp, n_dev
        self.nx = n_grp // 2
        ny = 1
        while 8 * ny * ny <= n_dev:
            ny *= 2
        self.ny, self.nz = ny, n_dev // ny
        self.team = n_grp * ny
        self.owned = rows // BS
        self.per = self.owned // n_grp
        self.n_blocks = self.owned * n_dev
        self.depth = 2 * npts // self.n_blocks
        self.steps = self.nz * self.per * self.depth // MSG
        self.zs = self.nz // self.steps
        self.nblk = self.zs * self.per
        self.line = (self.nx, self.ny, self.nz) == (2, 2, 4)
        self.fins = 2 if self.line else self.nz - 1


def kernel(
    cf,
    block_row, final_row, points_hbm, cent_hbm,
    distances, fresh_out,
    points, tab, slot_row, slot_col, out, recv, tgt_out, tgt_in,
    part, own_sum, agg_in, fin_in, cnt, cagg_in, cfin_in,
    dist, ret, xs, xin, tab_x, oth_sum, cnt_oth, x_out, x_in, cx_in,
    s_pts, r_pts, s_tgt, r_tgt, s_tab, r_tab, s_sum, r_agg, r_fin, s_cnt, r_cagg, r_cfin,
    s_ret, r_ret, s_x, r_x, s_side, r_side, s_cside, r_cside, in_sem,
):
    G, nx, ny, nz, TM = cf.g, cf.nx, cf.ny, cf.nz, cf.team
    per, depth, steps, zs, nblk = cf.per, cf.depth, cf.steps, cf.zs, cf.nblk
    g, d = lax.axis_index("grp"), lax.axis_index("dev")
    x, c = g // 2, g % 2
    z, y = d // ny, d % ny
    npts, width = points.shape
    share = width // G
    quarter = per * BS
    R = TM * MSG

    def to(gg, zz, yy):
        return {"grp": gg, "dev": zz * ny + yy}

    def split(o):
        return o // (2 * nx), o // 2 % nx, o % 2

    def near(s):
        return cf.line and s == steps - 1

    def mate(o, s=0):
        dy, dx, dc = split(o)
        return to((x + (0 if near(s) else dx)) % nx * 2 + (c + dc) % 2, z, (y + dy) % ny)

    def back(o, s):
        dy, dx, dc = split(o)
        return to((x + nx - (0 if near(s) else dx)) % nx * 2 + (c + dc) % 2, z, (y + ny - dy) % ny)

    def remote(s):
        return [o for o in range(TM) if (split(o)[0] or split(o)[2] if near(s) else o)]

    def start_of(xq, cq):
        return pl.multiple_of((cq * nx + xq) * quarter, quarter)

    def copy(src, dst, ss, rs, dev):
        return pltpu.make_async_remote_copy(
            src_ref=src, dst_ref=dst, send_sem=ss, recv_sem=rs, device_id=dev, device_id_type=MESH
        )

    half = z // (nz // 2)
    if cf.line:
        z_mate, z_inner, z_edge = half * 2 + 1 - z % 2, 2 - half, 3 * (1 - half)
        mid = (z + half) % 2
        inner = mid == 1
        edge = mid == 0
        order = [z_edge, mid * z_mate + (1 - mid) * z_inner, mid * z_inner + (1 - mid) * z_mate, z]

    def zq(q):
        return order[q] if cf.line else (z + q + 1) % nz

    load_tab = pltpu.make_async_copy(
        cent_hbm.at[pl.ds(start_of(x, c), quarter)], tab.at[z], in_sem.at[0]
    )
    load_points = pltpu.make_async_copy(points_hbm, points, in_sem.at[1])
    load_points.start()
    if cf.line:
        load_other = pltpu.make_async_copy(
            cent_hbm.at[pl.ds(start_of(1 - x, c), quarter)], tab_x, in_sem.at[2]
        )

    barrier = pltpu.get_barrier_semaphore()
    peers = [mate(o) for o in range(1, TM)] + [to(g, (z + k) % nz, y) for k in range(1, nz)]
    for p in peers:
        pl.semaphore_signal(barrier, inc=1, device_id=p, device_id_type=MESH)

    def tabc(k, zt, zd, p):
        piece = tab.at[zt, pl.ds(p * BS, BS)]
        return copy(piece, piece, s_tab.at[k, p], r_tab.at[zt, p], to(g, zd, y))

    def forward(kinds, p):
        if cf.line:

            @pl.when(inner)
            def _():
                for kind in kinds:
                    kind[p].wait_recv()
                    kind[p].start()

    b = block_row[...]
    hold, sub = b >> bits(cf.owned), b & (cf.owned - 1)
    zb, yb = hold >> bits(ny), hold & (ny - 1)
    gb, jb = sub >> bits(per), sub & (per - 1)
    ob = ((yb - y + ny) & (ny - 1)) * nx + (((gb & (nx - 1)) - x + nx) & (nx - 1))
    ob = ob * 2 + (((gb >> bits(nx)) - c + 2) & 1)
    if cf.line:
        hb = zb >> 1
        qb = jnp.where(hb == half, jnp.where(zb == z, 3, 2 - mid), ((zb + hb) & 1) * (1 + mid))
    else:
        qb = (zb - z - 1 + nz) & (nz - 1)
    place = ((qb >> bits(zs)) * TM + ob) * MSG + ((qb & (zs - 1)) * per + jb) * depth

    step = min(256, npts)
    before = (
        lax.broadcasted_iota(I32, (step, step), 0) < lax.broadcasted_iota(I32, (step, step), 1)
    ).astype(BF16)
    seen = jnp.zeros((cf.n_blocks, 1), F32)
    for t in range(npts // step):
        here = slice(t * step, (t + 1) * step)
        member = (lax.broadcasted_iota(I32, (cf.n_blocks, step), 0) == b[:, here]).astype(F32)
        prior = jnp.dot(member.astype(BF16), before, preferred_element_type=F32) + seen
        rank = jnp.sum(member * prior, axis=0, keepdims=True)
        seen = seen + jnp.sum(member, axis=1, keepdims=True)
        slot = place[:, here] + rank.astype(I32)
        slot_row[:, here] = slot
        slot_col[here, :] = jnp.transpose(jnp.broadcast_to(slot.astype(F32), (8, step)))
    want_row = jnp.broadcast_to((final_row[...] + 1).astype(F32), (8, npts)).astype(BF16)
    load_points.wait()
    load_tab.start()
    if cf.line:
        load_other.start()

    pts_c, tgt_c, ret_c = {}, {}, {}
    for s in range(steps):
        for o in remote(s):
            pts_c[s, o] = copy(out.at[s, o], recv.at[s, o], s_pts.at[s, o], r_pts.at[s, o], mate(o, s))
            tgt_c[s, o] = copy(tgt_out.at[s, o], tgt_in.at[s, o], s_tgt.at[s, o], r_tgt.at[s, o], mate(o, s))
            ret_c[s, o] = copy(dist.at[s, o], ret.at[s, o], s_ret.at[s, o], r_ret.at[s, o], back(o, s))

    def tile(s, lo, n=2):
        base = (s * TM + lo) * MSG
        hot = (lax.broadcasted_iota(I32, (n * MSG, npts), 0) + base == slot_row[...]).astype(BF16)
        pts = jnp.dot(hot, points[...], preferred_element_type=F32).astype(BF16)
        tg = nt(want_row, hot)
        for i in range(n):
            o = lo + i
            rows, lanes = pts[i * MSG : (i + 1) * MSG], tg[:, i * MSG : (i + 1) * MSG]
            if o in remote(s):
                out[s, o] = rows
                tgt_out[s, o] = lanes
            else:
                recv[s, o] = rows
                tgt_in[s, o] = lanes

    def send(s, lo, n=2):
        for o in range(lo, lo + n):
            if o in remote(s):
                tgt_c[s, o].start()
                pts_c[s, o].start()

    def pack(s):
        for lo in ([6, 2, 4, 0] if near(s) else [4, 6, 2, 0]) if cf.line else range(TM - 2, -1, -2):
            if (s, lo) != (0, first_lo):
                tile(s, lo)
                send(s, lo)

    first_lo = 4 if cf.line else TM - 2
    tile(0, first_lo, 1)
    pl.semaphore_wait(barrier, len(peers))
    send(0, first_lo, 1)
    tile(0, first_lo + 1, 1)
    send(0, first_lo + 1, 1)

    load_tab.wait()
    if cf.line:
        own_up = [tabc(0, z, z_mate, p) for p in range(per)]
        own_cross = [tabc(1, z, z_inner, p) for p in range(per)]
        f_mate = [tabc(2, z_mate, z_inner, p) for p in range(per)]
        f_inner = [tabc(3, z_inner, z_mate, p) for p in range(per)]
        f_edge = [tabc(4, z_edge, z_mate, p) for p in range(per)]
        for q in own_up:
            q.start()

        @pl.when(inner)
        def _():
            for q in own_cross:
                q.start()
    else:
        spread = [tabc(k, z, (z + k) % nz, p) for k in range(1, nz) for p in range(per)]
        for q in spread:
            q.start()

    def each(n, body):
        if n <= 2:
            for i in range(n):
                body(i)
        else:
            pl.loop(0, n)(body)

    ones = jnp.ones((8, R), BF16)

    def sums(s):
        for o in range(1, TM):
            tgt_c[s, o].wait_recv()
            pts_c[s, o].wait_recv()
        row = jnp.concatenate([tgt_in[s, o][0:1] for o in range(TM)], axis=1).astype(I32) - 1
        in_blk = (lax.broadcasted_iota(I32, (1, R), 1) & (MSG - 1)) >> bits(depth)

        def block(blk, own):
            want = jnp.where(in_blk == blk, row, -1)
            hot = (lax.broadcasted_iota(I32, (BS, R), 0) == want).astype(BF16)
            q, j = s * zs + blk // per, blk % per
            here = pl.ds(j * BS if isinstance(j, int) else pl.multiple_of(j * BS, BS), BS)
            cnt[q, j] = nt(ones, hot)
            total = jnp.dot(hot, recv[s].reshape(R, width), preferred_element_type=F32)
            if own:
                own_sum[here, :] = total
            else:
                part[q, here, :] = total.astype(BF16)

        n_own = per if s == steps - 1 else 0
        each(nblk - n_own, lambda blk: block(blk, False))
        for blk in range(nblk - n_own, nblk):
            block(blk, True)

    def distance(pts, table):
        cross = nt(pts, table)
        wide, twide = pts.astype(F32), table.astype(F32)
        rn = jnp.sum(wide * wide, axis=1, keepdims=True)
        cn = jnp.sum(twide * twide, axis=1, keepdims=True)
        cn = jnp.transpose(jnp.broadcast_to(cn, (BS, MSG)))[0:1]
        return ((rn - 2.0 * cross + cn) / width).astype(BF16)

    def give(s, units):
        far = remote(s)
        for o in [o for o in units if o in far]:
            ret_c[s, o].start()
        for o in units:
            if o not in far:
                ret[s, o] = dist[s, o]

    def dists(s):
        def block(blk):
            q, j = s * zs + blk // per, blk % per
            here = pl.ds(j * BS if isinstance(j, int) else pl.multiple_of(j * BS, BS), BS)
            rows = pl.ds(blk * depth if isinstance(blk, int) else pl.multiple_of(blk * depth, depth), depth)
            pts = recv[s, :, rows, :].reshape(TM * depth, width)
            dist[s, :, rows, :] = distance(pts, tab[zq(q), here, :]).reshape(TM, depth, BS)

        each(nblk, block)
        give(s, list(range(2, TM)) + [0, 1])

    def both(ref, s, dx, *rest):
        return jnp.concatenate([ref[(s, slice(u, u + 2)) + rest] for u in range(dx * 2, TM, 2 * nx)], axis=0)

    def near_sums(s, dx):
        units = [u + dc for u in range(dx * 2, TM, 2 * nx) for dc in range(2)]
        for o in units:
            if o in remote(s):
                tgt_c[s, o].wait_recv()
                pts_c[s, o].wait_recv()
        n = len(units) * MSG
        row = jnp.concatenate([tgt_in[s, o][0:1] for o in units], axis=1).astype(I32) - 1
        in_blk = (lax.broadcasted_iota(I32, (1, n), 1) & (MSG - 1)) >> bits(depth)
        for j in range(per):
            want = jnp.where(in_blk == j, row, -1)
            hot = (lax.broadcasted_iota(I32, (BS, n), 0) == want).astype(BF16)
            many = nt(jnp.ones((8, n), BF16), hot)
            total = jnp.dot(hot, both(recv, s, dx).reshape(n, width), preferred_element_type=F32)
            if dx:
                cnt_oth[j] = many
                oth_sum[j * BS : (j + 1) * BS, :] = total
            else:
                cnt[nz - 1, j] = many
                own_sum[j * BS : (j + 1) * BS, :] = total

    def near_dists(s, dx):
        for j in range(per):
            here, rows = slice(j * BS, (j + 1) * BS), slice(j * depth, (j + 1) * depth)
            pts = both(recv, s, dx, rows).reshape(-1, width)
            table = tab_x[here, :] if dx else tab[z, here, :]
            res = distance(pts, table).reshape(-1, depth, BS)
            for i, u in enumerate(range(dx * 2, TM, 2 * nx)):
                dist[s, u : u + 2, rows, :] = res[2 * i : 2 * i + 2]
        give(s, [u + dc for u in range(dx * 2, TM, 2 * nx) for dc in range(2)])

    gathered = []

    def gather(s, lo, hi):
        for o in remote(s):
            if lo <= o < hi:
                ret_c[s, o].wait_recv()
        first = not gathered
        gathered.append(s)
        ptile = min(256, npts)
        n = (hi - lo) * MSG

        @pl.loop(0, npts // ptile, unroll=2)
        def _(t):
            here = pl.ds(pl.multiple_of(t * ptile, ptile), ptile)
            where = slot_col[here, 0:1].astype(I32)
            hot = (lax.broadcasted_iota(I32, (ptile, n), 1) + s * R + lo * MSG == where).astype(BF16)
            acc = jnp.dot(hot, ret[s, lo:hi].reshape(n, BS), preferred_element_type=F32)
            if not first:
                acc += distances[here, :].astype(F32)
            distances[here, :] = acc.astype(BF16)

    if cf.line:

        def pair(q, j, dst, cdst, rs, crs, zd):
            piece = pl.ds(j * BS, BS)
            return [
                copy(part.at[q, piece], dst.at[piece], s_sum.at[q, j], rs.at[j], to(g, zd, y)),
                copy(cnt.at[q, j], cdst.at[j], s_cnt.at[q, j], crs.at[j], to(g, zd, y)),
            ]

        def agg(q, j, k, zd):
            return pair(q, j, agg_in.at[k], cagg_in.at[k], r_agg.at[k], r_cagg.at[k], zd)

        def fin(q, j, k, zd):
            return pair(q, j, fin_in.at[k], cfin_in.at[k], r_fin.at[k], r_cfin.at[k], zd)

        edge_out, inner_out, inner_in = {}, {}, {}
        for j in range(per):
            edge_out[0, j], edge_out[1, j], edge_out[2, j] = agg(0, j, 0, z_mate), agg(1, j, 1, z_mate), fin(2, j, 0, z_mate)
            inner_out[0, j], inner_out[1, j], inner_out[2, j] = (
                agg(0, j, 2, z_inner), fin(1, j, 0, z_mate), fin(2, j, 1, z_inner)
            )
            inner_in[0, j], inner_in[1, j], inner_in[2, j] = agg(0, j, 0, z_mate), agg(1, j, 2, z_inner), agg(2, j, 1, z_mate)
        slot_of = [0, 2, 1]

        def lift(q):
            @pl.when(edge)
            def _():
                for j in range(per):
                    for k in edge_out[q, j]:
                        k.start()

        def merge(q, j):
            @pl.when(inner)
            def _():
                for k in inner_in[q, j]:
                    k.wait_recv()
                here = pl.ds(j * BS, BS)
                total = part[q, here, :].astype(F32) + agg_in[slot_of[q], here, :].astype(F32)
                part[q, here, :] = total.astype(BF16)
                cnt[q, j] = cnt[q, j] + cagg_in[slot_of[q], j]
                for k in inner_out[q, j]:
                    k.start()

        def tables(q):
            @pl.when(edge)
            def _():
                for p in range(per):
                    tabc(3, order[q], z, p).wait_recv()

        def arrive():
            for j in range(per):
                here = pl.ds(j * BS, BS)
                for k in edge_out[2, j]:
                    k.wait_recv()
                own_sum[here, :] += fin_in[0, here, :].astype(F32)
                cnt[nz - 1, j] = cnt[nz - 1, j] + cfin_in[0, j]

            @pl.when(inner)
            def _():
                for j in range(per):
                    here = pl.ds(j * BS, BS)
                    for k in inner_out[2, j]:
                        k.wait_recv()
                    own_sum[here, :] += fin_in[1, here, :].astype(F32)
                    cnt[nz - 1, j] = cnt[nz - 1, j] + cfin_in[1, j]

    else:
        direct = []
        for q in range(nz - 1):
            direct.append(copy(part.at[q], fin_in.at[q], s_sum.at[q, 0], r_fin.at[q, 0], to(g, zq(q), y)))
            direct.append(copy(cnt.at[q], cfin_in.at[q], s_cnt.at[q, 0], r_cfin.at[q, 0], to(g, zq(q), y)))

        def arrive():
            for q in direct:
                q.wait_recv()

    def group(k):
        dx, dc = k // 2, k % 2
        return (x + dx) % nx * 2 + (c + dc) % 2

    def settle(xq, cq, block):
        fresh_out[pl.ds(start_of(xq, cq), quarter), :] = block.astype(F32)

    if cf.line:
        side = 2 * share
        mine, theirs = (pl.ds(pl.multiple_of(k * side, side), side) for k in (x, 1 - x))
        across, beside = to((1 - x) * 2 + c, z, y), to(x * 2 + 1 - c, z, y)
        side_c = [
            [
                [
                    copy(x_out.at[k, j], x_in.at[k, j], s_side.at[k, j], r_side.at[k, j], across),
                    copy((cnt_oth if k else cnt.at[nz - 1]).at[j], cx_in.at[k, j], s_cside.at[k, j], r_cside.at[k, j], across),
                ]
                for j in range(per)
            ]
            for k in (0, 1)
        ]
        x_c = {k: copy(xs.at[(1 - c) * 2 + k], xin.at[k], s_x.at[k], r_x.at[k], beside) for k in (0, 1)}

        def cross(k):
            total = oth_sum if k else own_sum
            for j in range(per):
                here = pl.ds(j * BS, BS)
                x_out[k, j] = total[here, theirs].astype(BF16)
                for q in side_c[k][j]:
                    q.start()

        def finish(k):
            for j in range(per):
                for q in side_c[1 - k][j]:
                    q.wait_recv()
                here = pl.ds(j * BS, BS)
                total = oth_sum[here, mine] if k else own_sum[here, mine]
                old = tab_x[here, mine] if k else tab[z, here, mine]
                many = (cnt_oth[j] if k else cnt[nz - 1, j]) + cx_in[1 - k, j]
                many = 1.0 / (jnp.transpose(many)[:, 0:1] + 1.0)
                total = total + x_in[1 - k, j].astype(F32) + old.astype(F32)
                fresh = (total * many).astype(BF16)
                for i in range(2):
                    xs[i * 2 + k, here, :] = fresh[:, i * share : (i + 1) * share]
            x_c[k].start()
            settle((x + k) % 2, c, xs[c * 2 + k])

    else:
        x_c = {k: copy(xs.at[group(k)], xin.at[k - 1], s_x.at[k], r_x.at[k], to(group(k), z, y)) for k in range(1, G)}

        def finish():
            arrive()
            for j in range(per):
                here = pl.ds(j * BS, BS)
                total, many = own_sum[here, :], cnt[nz - 1, j]
                for f in range(cf.fins):
                    total += fin_in[f, here, :].astype(F32)
                    many += cfin_in[f, j]
                many = 1.0 / (jnp.transpose(many)[:, 0:1] + 1.0)
                fresh = ((total + tab[z, here, :].astype(F32)) * many).astype(BF16)
                for k in range(G):
                    xs[k, here, :] = fresh[:, k * share : (k + 1) * share]
            for k in list(range(2, G)) + [1]:
                x_c[k].start()

    if cf.line:
        pack(0)
        pack(1)
        pack(2)
        forward([f_mate, f_inner], 0)
        pack(3)
        for p in range(1, per):
            forward([f_mate, f_inner], p)
        sums(0)
        lift(0)
        for p in range(per):
            forward([f_edge], p)
        sums(1)
        lift(1)
        for j in range(per):
            merge(0, j)
        tables(1)
        dists(1)
        merge(1, 0)
        sums(2)
        lift(2)
        for j in range(1, per):
            merge(1, j)
        for j in range(per):
            merge(2, j)
        tables(0)
        tables(2)
        dists(0)
        dists(2)
        load_other.wait()
        near_sums(3, 1)
        cross(1)
        near_dists(3, 1)
        gather(1, 0, TM // 2)
        gather(0, 0, TM // 2)
        gather(2, 0, TM // 2)
        near_sums(3, 0)
        arrive()
        cross(0)
        near_dists(3, 0)
        gather(1, TM // 2, TM)
        finish(0)
        gather(0, TM // 2, TM)
        gather(3, 0, TM // 2)
        gather(2, TM // 2, TM)
        gather(3, TM - 2, TM)
        finish(1)
        gather(3, TM // 2, TM - 2)
        for k in (0, 1):
            x_c[k].wait_recv()
            settle((x + k) % 2, 1 - c, xin[k])
    else:
        for s in range(steps):
            pack(s)
        for s in range(steps):
            sums(s)
        for k in direct:
            k.start()
        for q in spread:
            q.wait_recv()
        for s in range(steps):
            dists(s)
        finish()
        for s in range(steps):
            gather(s, 0, TM)
        settle(x, c, xs[g])
        for k in range(1, G):
            x_c[k].wait_recv()
            dx, dc = k // 2, k % 2
            settle((x + nx - dx) % nx, (c + dc) % 2, xin[k - 1])

    for group_c in (pts_c, tgt_c, ret_c, x_c):
        for q in group_c.values():
            q.wait_send()
    if cf.line:
        for q in own_up:
            q.wait_send()
        for group_c in side_c[0] + side_c[1] + list(edge_out.values()):
            for q in group_c:
                q.wait_send()

        @pl.when(inner)
        def _():
            for q in own_cross + f_mate + f_inner + f_edge:
                q.wait_send()
    else:
        for q in spread + direct:
            q.wait_send()


def shards(points, blocks, finals, centroids):
    n_dev = lax.axis_size("dev")
    n_grp = lax.axis_size("grp")
    npts, width = points.shape
    rows = centroids.shape[0]
    cf = Sizes(n_grp, n_dev, npts, rows)
    share = width // n_grp
    quarter = cf.per * BS
    nz, tm, steps = cf.nz, cf.team, cf.steps

    dma = pltpu.SemaphoreType.DMA
    vm = pltpu.VMEM
    return pl.pallas_call(
        functools.partial(kernel, cf),
        out_shape=(vm((npts, BS), BF16), vm((rows, share), F32)),
        in_specs=[pl.BlockSpec(memory_space=vm)] * 2 + [pl.BlockSpec(memory_space=pl.ANY)] * 2,
        out_specs=(pl.BlockSpec(memory_space=vm),) * 2,
        scratch_shapes=[
            vm((npts, width), BF16),
            vm((nz, quarter, width), BF16),
            vm((1, npts), I32),
            vm((npts, 8), F32),
            vm((steps, tm, MSG, width), BF16),
            vm((steps, tm, MSG, width), BF16),
            vm((steps, tm, 8, MSG), F32),
            vm((steps, tm, 8, MSG), F32),
            vm((nz - 1, quarter, width), BF16),
            vm((quarter, width), F32),
            vm((3, quarter, width), BF16),
            vm((cf.fins, quarter, width), BF16),
            vm((nz, cf.per, 8, BS), F32),
            vm((3, cf.per, 8, BS), F32),
            vm((cf.fins, cf.per, 8, BS), F32),
            vm((steps, tm, MSG, BS), BF16),
            vm((steps, tm, MSG, BS), BF16),
            vm((n_grp, quarter, share), BF16),
            vm((n_grp - 1, quarter, share), BF16),
            vm((quarter, width), BF16),
            vm((quarter, width), F32),
            vm((cf.per, 8, BS), F32),
            vm((2, cf.per, BS, 2 * share), BF16),
            vm((2, cf.per, BS, 2 * share), BF16),
            vm((2, cf.per, 8, BS), F32),
            dma((steps, tm)), dma((steps, tm)), dma((steps, tm)), dma((steps, tm)),
            dma((max(5, nz), cf.per)), dma((nz, cf.per)),
            dma((nz - 1, cf.per)), dma((3, cf.per)), dma((cf.fins, cf.per)), dma((nz - 1, cf.per)), dma((3, cf.per)), dma((cf.fins, cf.per)),
            dma((steps, tm)), dma((steps, tm)), dma((n_grp,)), dma((n_grp,)),
            dma((2, cf.per)), dma((2, cf.per)), dma((2, cf.per)), dma((2, cf.per)), dma((3,)),
        ],
        compiler_params=pltpu.CompilerParams(
            collective_id=0, has_side_effects=True, vmem_limit_bytes=58_000_000
        ),
    )(blocks.reshape(1, npts), finals.reshape(1, npts), points, centroids)


def solution(mesh):
    placed = (P(("grp", "dev"), None), P(("grp", "dev"), None), P(("grp", "dev")), P("dev", None))
    return jax.shard_map(
        shards,
        mesh=mesh,
        in_specs=placed,
        out_specs=(P(("grp", "dev"), None), P("dev", "grp")),
        check_vma=False,
    )
```
